32 devices in a mesh: seq: 4 (over z), tp: 4 (over y, x), dp: 2 (over core).
Axes of the slice: x: 2, y: 2, z: 4, core: 2. Of those that a mesh axis runs over, the one named last changes fastest.
Arguments:
- x_ckpt: bfloat16 [1024, 5120], P(('dp', 'seq', 'tp')), parts along dimension 0, may hold values from -5 to 5
- bc_ckpt: bfloat16 [2, 1024, 128], P(None, ('dp', 'seq', 'tp')), parts along dimension 1, may hold values from -1 to 1
- step_sizes: float32 [80, 1024], P('tp', ('dp', 'seq')), parts along dimension 1, may hold values from 0.03 to 0.3
- decay_rate: float32 [80], P('tp'), may hold values from 0 to 1, as said below
- skip_gain: float32 [80], P('tp'), may hold values from 0.25 to 1.75
- grad_out: bfloat16 [1024, 5120], P(('dp', 'seq'), 'tp'), parts along dimension 0, may hold values from -3 to 3
Outputs:
- grad_x: bfloat16 [1024, 5120], P(('dp', 'seq'), 'tp'), parts along dimension 0
- grad_bc: float32 [2, 1024, 128], P(None, ('dp', 'seq', 'tp')), parts along dimension 1
- grad_step: float32 [80, 1024], P('tp', ('dp', 'seq')), parts along dimension 1
The draws below stay inside these ranges and needn't reach their ends.
There are 2 independent parts, one for each index of `dp`. The reference program is written for one: setup_inputs(seed, part) draws one part's arguments, and reference() takes and returns one part's arrays. A program takes and returns all parts, laid end to end along the dimension named above; an argument that names none is the same for every part. Nothing has to cross between parts.
Inputs may be any that keep to these rules, and one draw needn't show every extreme that they name: `decay_rate`: positive decay rates of the 80 heads.
All inputs are finite; a program needn't handle non-finite values.
Results may differ from the reference program's by a relative error of at most 0.001.
Values may be sent and summed in bfloat16 or wider, within the bound.
A program may use at most 128 MiB of HBM per device.

```python
import math
from functools import partial
import jax
import jax.numpy as jnp
from jax import lax

HEADS = 80
STATE = 128
BLOCK = 128
TOKENS = 512
INNER = 5120


def draw_decay_rate(key, part):
    rate_key = jax.random.fold_in(key, 11)
    top_rate = 0.5
    low_rate = 20.0 / TOKENS
    drawn = jax.random.uniform(rate_key, (HEADS,), minval=math.log(low_rate), maxval=math.log(top_rate))
    return jnp.exp(drawn).astype(jnp.float32)


def draw_step_sizes(key, part):
    level_key, factor_key = jax.random.split(jax.random.fold_in(key, 23))
    level = jnp.exp(jax.random.uniform(level_key, (HEADS, 1), minval=math.log(0.043), maxval=math.log(0.187)))
    factor = jnp.exp(jax.random.uniform(factor_key, (HEADS, TOKENS), minval=math.log(0.7), maxval=math.log(1.6)))
    return jnp.clip(level * factor, 0.03, 0.3).astype(jnp.float32)


def draw_bc_ckpt(key, part):
    sign_key, noise_key = jax.random.split(jax.random.fold_in(key, 37))
    direction = jnp.where(jax.random.bernoulli(sign_key, 0.5, (STATE,)), 1.0, -1.0)
    common = direction / (8.0 * math.sqrt(STATE))
    spread = 1.0 / math.sqrt(STATE)
    noise = jnp.clip(jax.random.normal(noise_key, (2, TOKENS, STATE)), -4.0, 4.0) * spread
    return jnp.clip(common[None, None, :] + noise, -1.0, 1.0).astype(jnp.bfloat16)


def draw_x_ckpt(key, part):
    offset_key, noise_key = jax.random.split(jax.random.fold_in(key, 41))
    offset = jnp.clip(0.8 * jax.random.normal(offset_key, (1, INNER)), -2.5, 2.5)
    noise = jnp.clip(0.6 * jax.random.normal(noise_key, (TOKENS, INNER)), -2.4, 2.4)
    return jnp.clip(offset + noise, -5.0, 5.0).astype(jnp.bfloat16)


def draw_grad_out(key, part):
    offset_key, noise_key = jax.random.split(jax.random.fold_in(key, 53))
    offset = jnp.clip(0.4 * jax.random.normal(offset_key, (1, INNER)), -1.5, 1.5)
    noise = jnp.clip(0.4 * jax.random.normal(noise_key, (TOKENS, INNER)), -1.5, 1.5)
    return jnp.clip(offset + noise, -3.0, 3.0).astype(jnp.bfloat16)


def setup_inputs(seed: int = 0, part: int = 0) -> dict:
    key_of = jax.random.split(jax.random.key(seed), 7)
    part_splits = jax.random.split(jax.random.fold_in(key_of[6], part), 7)
    return {
        "x_ckpt": draw_x_ckpt(jax.random.fold_in(jax.random.fold_in(key_of[6], part), 71), part),
        "bc_ckpt": draw_bc_ckpt(jax.random.fold_in(jax.random.fold_in(key_of[6], part), 71), part),
        "step_sizes": draw_step_sizes(jax.random.fold_in(jax.random.fold_in(key_of[6], part), 71), part),
        "decay_rate": draw_decay_rate(jax.random.fold_in(key_of[6], 71), part),
        "skip_gain": jnp.clip(1.0 + 0.15 * jax.random.normal(key_of[4], (HEADS,), jnp.float32), 0.25, 1.75),
        "grad_out": draw_grad_out(jax.random.fold_in(jax.random.fold_in(key_of[6], part), 71), part),
    }


highest = lax.Precision.HIGHEST

def block_step(head_rates, head_gains, carry_state, pieces):
    inputs, step_block, proj_b, proj_c = pieces
    head_count = step_block.shape[0]
    row_count = step_block.shape[1]
    values = inputs.astype(jnp.float32).reshape(row_count, head_count, -1)
    cumulative = jnp.cumsum(-head_rates[:, None] * step_block, axis=1)
    positions = jnp.arange(row_count, dtype=jnp.int32)
    causal = positions[:, None] >= positions[None, :]
    log_gaps = cumulative[:, :, None] - cumulative[:, None, :]
    within = jnp.where(causal, jnp.exp(jnp.where(causal, log_gaps, 0.0)), 0.0)
    scores = jnp.dot(proj_c, proj_b.T, precision=highest, preferred_element_type=jnp.float32)
    weights = within * scores[None, :, :] * step_block[:, None, :]
    local_part = jnp.einsum('hts,shp->thp', weights, values, precision=highest, preferred_element_type=jnp.float32)
    carried = jnp.einsum('tn,hpn->thp', proj_c, carry_state, precision=highest, preferred_element_type=jnp.float32)
    carried = carried * jnp.exp(cumulative).T[:, :, None]
    result = local_part + carried + head_gains[None, :, None] * values
    tail_weight = jnp.exp(cumulative[:, -1:] - cumulative) * step_block
    fresh_state = jnp.einsum('hs,shp,sn->hpn', tail_weight, values, proj_b, precision=highest, preferred_element_type=jnp.float32)
    final_state = jnp.exp(cumulative[:, -1])[:, None, None] * carry_state + fresh_state
    return (final_state, result.reshape(row_count, -1))

def run_blocks(inputs, step_sizes, proj_b, proj_c, start_state, head_rates, head_gains, block_rows):
    row_count = inputs.shape[0]
    block_count = row_count // block_rows
    head_count = step_sizes.shape[0]
    input_blocks = inputs.reshape(block_count, block_rows, inputs.shape[1])
    step_blocks = step_sizes.reshape(head_count, block_count, block_rows).transpose(1, 0, 2)
    b_blocks = proj_b.reshape(block_count, block_rows, proj_b.shape[1])
    c_blocks = proj_c.reshape(block_count, block_rows, proj_c.shape[1])
    stepper = jax.checkpoint(partial(block_step, head_rates, head_gains))
    final_state, results = lax.scan(stepper, start_state, (input_blocks, step_blocks, b_blocks, c_blocks))
    return (results.reshape(row_count, -1), final_state)

def reference(x_ckpt, bc_ckpt, step_sizes, decay_rate, skip_gain, grad_out):
    head_count = decay_rate.shape[0]
    head_width = x_ckpt.shape[1] // head_count
    proj_b = bc_ckpt[0].astype(jnp.float32)
    proj_c = bc_ckpt[1].astype(jnp.float32)
    start_state = jnp.zeros((head_count, head_width, proj_b.shape[1]), jnp.float32)

    def forward(inputs, basis_b, basis_c, step_block):
        output, final_state = run_blocks(inputs, step_block, basis_b, basis_c, start_state, decay_rate, skip_gain, BLOCK)
        return output
    output, pull_back = jax.vjp(forward, x_ckpt, proj_b, proj_c, step_sizes)
    grad_x, grad_b, grad_c, grad_step = pull_back(grad_out.astype(jnp.float32))
    return (grad_x, jnp.stack([grad_b, grad_c]), grad_step)
```

```python
from functools import partial

import jax
import jax.numpy as jnp
from jax import lax
from jax.experimental import pallas as pl
from jax.experimental.pallas import tpu as pltpu
from jax.sharding import PartitionSpec as P

MESH = pl.DeviceIdType.MESH
F32 = jnp.float32
BF16 = jnp.bfloat16
HEAD_PAD = 32
SKEW = 2

NN = (((1,), (0,)), ((), ()))
NT = (((1,), (1,)), ((), ()))


def dot(a, b, dims=NN):
    return lax.dot_general(a, b, dims, preferred_element_type=F32)


def exact(a, b):
    return lax.dot_general(
        a, b, NN, precision=lax.Precision.HIGHEST, preferred_element_type=F32
    )


def split(v):
    high = v.astype(BF16)
    return high, (v - high.astype(F32)).astype(BF16)


def dot2(a, b, dims=NN):
    return dot(a, b[0], dims) + dot(a, b[1], dims)


def dot2l(a, b, dims=NN):
    return dot(a[0], b, dims) + dot(a[1], b, dims)


def dot3(a, b, dims=NN):
    return dot(a[0], b[0], dims) + (dot(a[0], b[1], dims) + dot(a[1], b[0], dims))


def kernel(
    peers, blocks, head_width,
    x_ref, bc_ref, step_ref, rate_ref, gain_ref, dy_ref,
    gx_ref, gbc_ref, gstep_ref,
    xr, bcr, part, rs,
    state_in, state_out, pull_in, pull_out, fresh, pulled, a2_loc, z_loc,
    xs_h, xs_l, ys_h, ys_l, xc, dyc, ec, ed, gain_row,
    stp, rates, gains, cums, mt_acc, bc_acc, dcum_acc, dir_acc, sm, bcm,
    send_x, recv_x, send_b, recv_b, own_sem,
    send_f, recv_f, send_g, recv_g, send_r, recv_r,
):
    me = lax.axis_index("tp")
    block = lax.axis_index("seq")
    head_count, tokens = step_ref.shape
    width = dy_ref.shape[1]
    rows = x_ref.shape[0]
    chunks, _, lanes = xc.shape
    chunk_heads = lanes // head_width

    has_prev = block > 0
    has_next = block < blocks - 1

    barrier = pltpu.get_barrier_semaphore()
    for d in range(1, peers):
        pl.semaphore_signal(
            barrier, inc=1, device_id={"tp": lax.rem(me + d, peers)}, device_id_type=MESH
        )

    @pl.when(has_prev)
    def _():
        pl.semaphore_signal(barrier, inc=1, device_id={"seq": block - 1}, device_id_type=MESH)

    @pl.when(has_next)
    def _():
        pl.semaphore_signal(barrier, inc=1, device_id={"seq": block + 1}, device_id_type=MESH)

    neighbours = jnp.where(has_prev, 1, 0) + jnp.where(has_next, 1, 0)
    pl.semaphore_wait(barrier, peers - 1 + neighbours)

    def bc_copy(peer, slot):
        return pltpu.make_async_remote_copy(
            src_ref=bc_ref, dst_ref=bcr.at[slot],
            send_sem=send_b.at[peer], recv_sem=recv_b.at[slot],
            device_id={"tp": peer}, device_id_type=MESH,
        )

    def x_copy(peer, slot):
        return pltpu.make_async_remote_copy(
            src_ref=x_ref.at[:, pl.ds(pl.multiple_of(peer * width, 128), width)],
            dst_ref=xr.at[slot],
            send_sem=send_x.at[peer], recv_sem=recv_x.at[slot],
            device_id={"tp": peer}, device_id_type=MESH,
        )

    for d in range(1, peers):
        bc_copy(lax.rem(me + d, peers), me).start()
    for d in range(1, peers):
        x_copy(lax.rem(me + d, peers), me).start()
    own_x = pltpu.make_async_copy(
        x_ref.at[:, pl.ds(pl.multiple_of(me * width, 128), width)], xr.at[me], own_sem.at[0]
    )
    own_bc = pltpu.make_async_copy(bc_ref, bcr.at[me], own_sem.at[1])
    own_x.start()
    own_bc.start()

    stp[...] = jnp.zeros_like(stp)
    stp[0:head_count] = step_ref[...]
    rates[...] = jnp.zeros_like(rates)
    gains[...] = jnp.zeros_like(gains)
    for h in range(head_count):
        rates[h : h + 1] = jnp.full((1, tokens), rate_ref[h], F32)
        gains[h : h + 1] = jnp.full((1, tokens), gain_ref[h], F32)
    row = lax.broadcasted_iota(jnp.int32, (tokens, tokens), 0)
    col = lax.broadcasted_iota(jnp.int32, (tokens, tokens), 1)
    upto = row <= col
    cum = exact(-rates[...] * stp[...], jnp.where(upto, 1.0, 0.0).astype(F32))
    cums[...] = cum
    stacked = jnp.concatenate(
        [jnp.exp(cum), jnp.exp(-cum) * stp[...], gains[...], jnp.zeros_like(cum)], axis=0
    )
    table = split(stacked.T)
    pick_row = lax.broadcasted_iota(jnp.int32, (4 * HEAD_PAD, lanes), 0)
    pick_head = lax.broadcasted_iota(jnp.int32, (4 * HEAD_PAD, lanes), 1) // head_width
    for c in range(chunks):
        def spread(q):
            hit = pick_row == (q * HEAD_PAD + c * chunk_heads) + pick_head
            return jnp.where(hit, 1.0, 0.0).astype(BF16)

        grown = dot2l(table, spread(0))
        ec[c] = grown
        ed[c] = dot2l(table, spread(1))
        gain_row[c] = dot2l((table[0][0:16], table[1][0:16]), spread(2))[0:8]
        dy = dy_ref[:, c * lanes : (c + 1) * lanes]
        dyc[c] = dy
        high, low = split(grown * dy.astype(F32))
        ys_h[c] = high
        ys_l[c] = low

    own_bc.wait()
    for d in range(1, peers):
        source = lax.rem(me + d, peers)
        bc_copy(source, source).wait_recv()
    proj_b = bcr[:, 0].reshape(tokens, -1)
    proj_c = bcr[:, 1].reshape(tokens, -1)
    bcm[0] = proj_b
    bcm[1] = proj_c
    b_t = proj_b.astype(F32).T.astype(BF16)
    c_t = proj_c.astype(F32).T.astype(BF16)
    scores_t = jnp.where(upto, dot(proj_b, proj_c, NT), 0.0)
    sm[0], sm[1] = split(scores_t)
    sm[2], sm[3] = split(scores_t.T)
    for c in range(chunks):
        pulled[c] = dot2(c_t, (ys_h[c], ys_l[c]))

    @pl.when(jnp.logical_not(has_prev))
    def _():
        state_in[...] = jnp.zeros_like(state_in)

    @pl.when(jnp.logical_not(has_next))
    def _():
        pull_in[...] = jnp.zeros_like(pull_in)

    mt_acc[...] = jnp.zeros_like(mt_acc)
    bc_acc[...] = jnp.zeros_like(bc_acc)
    dcum_acc[...] = jnp.zeros_like(dcum_acc)
    dir_acc[...] = jnp.zeros_like(dir_acc)

    own_x.wait()
    for d in range(1, peers):
        source = lax.rem(me + d, peers)
        x_copy(source, source).wait_recv()
    for c in range(chunks):
        x = xr[:, :, c * lanes : (c + 1) * lanes].reshape(tokens, lanes)
        xc[c] = x
        pair = split(ed[c] * x.astype(F32))
        xs_h[c] = pair[0]
        xs_l[c] = pair[1]
        fresh[c] = dot2(b_t, pair)

    def forward_copy(c):
        return pltpu.make_async_remote_copy(
            src_ref=state_out.at[c], dst_ref=state_in.at[c],
            send_sem=send_f.at[c], recv_sem=recv_f.at[c],
            device_id={"seq": block + 1}, device_id_type=MESH,
        )

    def backward_copy(c):
        return pltpu.make_async_remote_copy(
            src_ref=pull_out.at[c], dst_ref=pull_in.at[c],
            send_sem=send_g.at[c], recv_sem=recv_g.at[c],
            device_id={"seq": block - 1}, device_id_type=MESH,
        )

    def selector(c):
        head = lax.broadcasted_iota(jnp.int32, (HEAD_PAD, lanes), 0)
        of = lax.broadcasted_iota(jnp.int32, (HEAD_PAD, lanes), 1) // head_width
        return jnp.where(head == c * chunk_heads + of, 1.0, 0.0).astype(BF16)

    def total_decay(c):
        return ec[c, tokens - 1 : tokens, :]

    def step(s, carry):
        cf = s - SKEW * block
        cb = s - SKEW * (blocks - 1 - block)
        do_f = jnp.logical_and(cf >= 0, cf < chunks)
        do_b = jnp.logical_and(cb >= 0, cb < chunks)

        @pl.when(do_f)
        def _():
            @pl.when(has_prev)
            def _():
                forward_copy(cf).wait_recv()

            state_out[cf] = total_decay(cf) * (state_in[cf] + fresh[cf])

            @pl.when(has_next)
            def _():
                forward_copy(cf).start()

        @pl.when(do_b)
        def _():
            @pl.when(has_next)
            def _():
                backward_copy(cb).wait_recv()

            @pl.when(has_prev)
            def _():
                pull_out[cb] = total_decay(cb) * pull_in[cb] + pulled[cb]
                backward_copy(cb).start()

        @pl.when(s < chunks)
        def _():
            xs = (xs_h[s], xs_l[s])
            ys = (ys_h[s], ys_l[s])
            a2_loc[s] = dot3((sm[0], sm[1]), ys)
            z_loc[s] = dot3((sm[2], sm[3]), xs)
            mt_acc[...] += dot3(xs, ys, NT)

        @pl.when(do_f)
        def _():
            entering = split(state_in[cf])
            z = z_loc[cf] + dot2(bcm[1], entering)
            bc_acc[1] += dot3((ys_h[cf], ys_l[cf]), entering, NT)
            v = split(ec[cf] * dyc[cf].astype(F32) * z)
            dcum_acc[...] += dot2(selector(cf), v, NT)

        @pl.when(do_b)
        def _():
            leaving = split(total_decay(cb) * pull_in[cb])
            a2 = a2_loc[cb] + dot2(bcm[0], leaving)
            bc_acc[0] += dot3((xs_h[cb], xs_l[cb]), leaving, NT)
            x = xc[cb].astype(F32)
            growth = ed[cb]
            gx = growth * a2 + gain_row[cb, 0:1, :] * dyc[cb].astype(F32)
            gx_ref[:, pl.ds(pl.multiple_of(cb * lanes, 128), lanes)] = gx.astype(BF16)
            direct = x * a2
            pick = selector(cb)
            dir_acc[...] += dot2(pick, split(direct), NT)
            dcum_acc[...] -= dot2(pick, split(growth * direct), NT)

        return carry

    lax.fori_loop(0, chunks + SKEW * (blocks - 1), step, 0)

    inner = jnp.where(upto, mt_acc[...], 0.0)
    grad_b = bc_acc[0] + dot2l(split(inner), bcm[1])
    grad_c = bc_acc[1] + dot2l(split(inner.T), bcm[0])
    for j in range(peers):
        part[j, 0] = grad_b[j * rows : (j + 1) * rows]
        part[j, 1] = grad_c[j * rows : (j + 1) * rows]

    def sum_copy(peer, slot):
        return pltpu.make_async_remote_copy(
            src_ref=part.at[peer], dst_ref=rs.at[slot],
            send_sem=send_r.at[peer], recv_sem=recv_r.at[slot],
            device_id={"tp": peer}, device_id_type=MESH,
        )

    for d in range(1, peers):
        sum_copy(lax.rem(me + d, peers), me).start()

    edge = jnp.zeros((HEAD_PAD, 8), F32)
    for c in range(chunks):
        both = (pull_in[c] * state_out[c]).reshape(-1, 8, lanes).sum(axis=0)
        edge = edge + dot2(selector(c), split(both), NT)
    edge = jnp.sum(edge, axis=1, keepdims=True)
    after = exact(dcum_acc[...], jnp.where(row >= col, 1.0, 0.0).astype(F32)) + edge
    gstep = jnp.exp(-cums[...]) * dir_acc[...] - rates[...] * after
    gstep_ref[...] = gstep[0:head_count]

    total = part[me]
    for d in range(1, peers):
        source = lax.rem(me + d, peers)
        sum_copy(source, source).wait_recv()
        total = total + rs[source]
    gbc_ref[...] = total

    for d in range(1, peers):
        peer = lax.rem(me + d, peers)
        bc_copy(peer, me).wait_send()
        x_copy(peer, me).wait_send()
        sum_copy(peer, me).wait_send()

    def drain(c, carry):
        @pl.when(has_next)
        def _():
            forward_copy(c).wait_send()

        @pl.when(has_prev)
        def _():
            backward_copy(c).wait_send()

        return carry

    lax.fori_loop(0, chunks, drain, 0)


def shards(x_ckpt, bc_ckpt, step_sizes, decay_rate, skip_gain, grad_out):
    peers, blocks = lax.axis_size("tp"), lax.axis_size("seq")
    rows = x_ckpt.shape[0]
    head_count, tokens = step_sizes.shape
    width = grad_out.shape[1]
    state = bc_ckpt.shape[2]
    lanes = 128
    chunks = width // lanes
    head_width = width // head_count
    wide = lambda dtype, size: pltpu.VMEM((chunks, size, lanes), dtype)
    dma = lambda n: pltpu.SemaphoreType.DMA((n,))
    vmem = pl.BlockSpec(memory_space=pltpu.VMEM)
    smem = pl.BlockSpec(memory_space=pltpu.SMEM)
    heads = pltpu.VMEM((HEAD_PAD, tokens), F32)
    return pl.pallas_call(
        partial(kernel, peers, blocks, head_width),
        out_shape=(
            jax.ShapeDtypeStruct((tokens, width), BF16),
            jax.ShapeDtypeStruct((2, rows, state), F32),
            jax.ShapeDtypeStruct((head_count, tokens), F32),
        ),
        in_specs=[vmem, vmem, vmem, smem, smem, vmem],
        out_specs=(vmem, vmem, vmem),
        scratch_shapes=[
            pltpu.VMEM((peers, rows, width), BF16),
            pltpu.VMEM((peers, 2, rows, state), BF16),
            pltpu.VMEM((peers, 2, rows, state), F32),
            pltpu.VMEM((peers, 2, rows, state), F32),
            *[wide(F32, state)] * 6,
            *[wide(F32, tokens)] * 2,
            *[wide(BF16, tokens)] * 6,
            *[wide(F32, tokens)] * 2,
            wide(F32, 8),
            heads, heads, heads, heads,
            pltpu.VMEM((tokens, tokens), F32),
            pltpu.VMEM((2, tokens, state), F32),
            heads, heads,
            pltpu.VMEM((4, tokens, tokens), BF16),
            pltpu.VMEM((2, tokens, state), BF16),
            dma(peers), dma(peers), dma(peers), dma(peers), dma(2),
            dma(chunks), dma(chunks), dma(chunks), dma(chunks),
            dma(peers), dma(peers),
        ],
        compiler_params=pltpu.CompilerParams(collective_id=0, has_side_effects=True),
    )(x_ckpt, bc_ckpt, step_sizes, decay_rate, skip_gain, grad_out)


def solution(mesh):
    return jax.shard_map(
        shards,
        mesh=mesh,
        in_specs=(
            P(("dp", "seq", "tp"), None),
            P(None, ("dp", "seq", "tp"), None),
            P("tp", ("dp", "seq")),
            P("tp"),
            P("tp"),
            P(("dp", "seq"), "tp"),
        ),
        out_specs=(
            P(("dp", "seq"), "tp"),
            P(None, ("dp", "seq", "tp"), None),
            P("tp", ("dp", "seq")),
        ),
        check_vma=False,
    )
```

```python
from functools import partial

import jax
import jax.numpy as jnp
from jax import lax
from jax.experimental import pallas as pl
from jax.experimental.pallas import tpu as pltpu
from jax.sharding import PartitionSpec as P

MESH = pl.DeviceIdType.MESH
F32 = jnp.float32
BF16 = jnp.bfloat16
HEAD_PAD = 32
SKEW = 2

NN = (((1,), (0,)), ((), ()))
NT = (((1,), (1,)), ((), ()))


def dot(a, b, dims=NN):
    return lax.dot_general(a, b, dims, preferred_element_type=F32)


def exact(a, b):
    return lax.dot_general(
        a, b, NN, precision=lax.Precision.HIGHEST, preferred_element_type=F32
    )


def split(v):
    high = v.astype(BF16)
    return high, (v - high.astype(F32)).astype(BF16)


def joined(a, b, dims=NN):
    return dot(jnp.concatenate(a, axis=1), jnp.concatenate(b, axis=dims[0][1][0]), dims)


def dot2(a, b, dims=NN):
    return joined((a, a), b, dims)


def dot2l(a, b, dims=NN):
    return joined(a, (b, b), dims)


def dot3(a, b, dims=NN):
    return joined((a[0], a[0], a[1]), (b[0], b[1], b[0]), dims)


def kernel(
    peers, blocks, head_width,
    x_ref, bc_ref, step_ref, rate_ref, gain_ref, dy_ref,
    gx_ref, gbc_ref, gstep_ref,
    xr, bcr, part, rs,
    state_in, state_out, pull_in, pull_out, fresh, pulled,
    xs_h, xs_l, ys_h, ys_l, xc, dyc, ec, ed, gain_row,
    stp, rates, gains, cums, mt_acc, bc_acc, dcum_acc, dir_acc, sm, bcm,
    send_x, recv_x, send_b, recv_b, own_sem,
    send_f, recv_f, send_g, recv_g, send_r, recv_r,
):
    me = lax.axis_index("tp")
    block = lax.axis_index("seq")
    head_count, tokens = step_ref.shape
    width = dy_ref.shape[1]
    rows = x_ref.shape[0]
    chunks, _, lanes = xc.shape
    chunk_heads = lanes // head_width

    has_prev = block > 0
    has_next = block < blocks - 1

    barrier = pltpu.get_barrier_semaphore()
    for d in range(1, peers):
        pl.semaphore_signal(
            barrier, inc=1, device_id={"tp": lax.rem(me + d, peers)}, device_id_type=MESH
        )

    @pl.when(has_prev)
    def _():
        pl.semaphore_signal(barrier, inc=1, device_id={"seq": block - 1}, device_id_type=MESH)

    @pl.when(has_next)
    def _():
        pl.semaphore_signal(barrier, inc=1, device_id={"seq": block + 1}, device_id_type=MESH)

    neighbours = jnp.where(has_prev, 1, 0) + jnp.where(has_next, 1, 0)
    pl.semaphore_wait(barrier, peers - 1 + neighbours)

    def bc_copy(peer, slot):
        return pltpu.make_async_remote_copy(
            src_ref=bc_ref, dst_ref=bcr.at[slot],
            send_sem=send_b.at[peer], recv_sem=recv_b.at[slot],
            device_id={"tp": peer}, device_id_type=MESH,
        )

    def x_copy(peer, slot):
        return pltpu.make_async_remote_copy(
            src_ref=x_ref.at[:, pl.ds(pl.multiple_of(peer * width, 128), width)],
            dst_ref=xr.at[slot],
            send_sem=send_x.at[peer], recv_sem=recv_x.at[slot],
            device_id={"tp": peer}, device_id_type=MESH,
        )

    for d in range(1, peers):
        bc_copy(lax.rem(me + d, peers), me).start()
    for d in range(1, peers):
        x_copy(lax.rem(me + d, peers), me).start()
    own_x = pltpu.make_async_copy(
        x_ref.at[:, pl.ds(pl.multiple_of(me * width, 128), width)], xr.at[me], own_sem.at[0]
    )
    own_bc = pltpu.make_async_copy(bc_ref, bcr.at[me], own_sem.at[1])
    own_x.start()
    own_bc.start()

    stp[...] = jnp.zeros_like(stp)
    stp[0:head_count] = step_ref[...]
    rates[...] = jnp.zeros_like(rates)
    gains[...] = jnp.zeros_like(gains)
    for h in range(head_count):
        rates[h : h + 1] = jnp.full((1, tokens), rate_ref[h], F32)
        gains[h : h + 1] = jnp.full((1, tokens), gain_ref[h], F32)
    row = lax.broadcasted_iota(jnp.int32, (tokens, tokens), 0)
    col = lax.broadcasted_iota(jnp.int32, (tokens, tokens), 1)
    upto = row <= col
    cum = exact(-rates[...] * stp[...], jnp.where(upto, 1.0, 0.0).astype(F32))
    cums[...] = cum
    stacked = jnp.concatenate(
        [jnp.exp(cum), jnp.exp(-cum) * stp[...], gains[...], jnp.zeros_like(cum)], axis=0
    )
    table = split(stacked.T)
    pick_row = lax.broadcasted_iota(jnp.int32, (4 * HEAD_PAD, lanes), 0)
    pick_head = lax.broadcasted_iota(jnp.int32, (4 * HEAD_PAD, lanes), 1) // head_width
    for c in range(chunks):
        def spread(q):
            hit = pick_row == (q * HEAD_PAD + c * chunk_heads) + pick_head
            return jnp.where(hit, 1.0, 0.0).astype(BF16)

        grown = dot2l(table, spread(0))
        ec[c] = grown
        ed[c] = dot2l(table, spread(1))
        gain_row[c] = dot2l((table[0][0:16], table[1][0:16]), spread(2))[0:8]
        dy = dy_ref[:, c * lanes : (c + 1) * lanes]
        dyc[c] = dy
        high, low = split(grown * dy.astype(F32))
        ys_h[c] = high
        ys_l[c] = low

    own_bc.wait()
    for d in range(1, peers):
        source = lax.rem(me + d, peers)
        bc_copy(source, source).wait_recv()
    proj_b = bcr[:, 0].reshape(tokens, -1)
    proj_c = bcr[:, 1].reshape(tokens, -1)
    bcm[0] = proj_b
    bcm[1] = proj_c
    b_t = proj_b.astype(F32).T.astype(BF16)
    c_t = proj_c.astype(F32).T.astype(BF16)
    scores_t = jnp.where(upto, dot(proj_b, proj_c, NT), 0.0)
    sm[0], sm[1] = split(scores_t)
    sm[2], sm[3] = split(scores_t.T)
    for c in range(chunks):
        pulled[c] = dot2(c_t, (ys_h[c], ys_l[c]))

    @pl.when(jnp.logical_not(has_prev))
    def _():
        state_in[...] = jnp.zeros_like(state_in)

    @pl.when(jnp.logical_not(has_next))
    def _():
        pull_in[...] = jnp.zeros_like(pull_in)

    mt_acc[...] = jnp.zeros_like(mt_acc)
    bc_acc[...] = jnp.zeros_like(bc_acc)
    dcum_acc[...] = jnp.zeros_like(dcum_acc)
    dir_acc[...] = jnp.zeros_like(dir_acc)

    own_x.wait()
    for d in range(1, peers):
        source = lax.rem(me + d, peers)
        x_copy(source, source).wait_recv()
    for c in range(chunks):
        x = xr[:, :, c * lanes : (c + 1) * lanes].reshape(tokens, lanes)
        xc[c] = x
        pair = split(ed[c] * x.astype(F32))
        xs_h[c] = pair[0]
        xs_l[c] = pair[1]
        fresh[c] = dot2(b_t, pair)

    def forward_copy(c):
        return pltpu.make_async_remote_copy(
            src_ref=state_out.at[c], dst_ref=state_in.at[c],
            send_sem=send_f.at[c], recv_sem=recv_f.at[c],
            device_id={"seq": block + 1}, device_id_type=MESH,
        )

    def backward_copy(c):
        return pltpu.make_async_remote_copy(
            src_ref=pull_out.at[c], dst_ref=pull_in.at[c],
            send_sem=send_g.at[c], recv_sem=recv_g.at[c],
            device_id={"seq": block - 1}, device_id_type=MESH,
        )

    def selector(c):
        head = lax.broadcasted_iota(jnp.int32, (HEAD_PAD, lanes), 0)
        of = lax.broadcasted_iota(jnp.int32, (HEAD_PAD, lanes), 1) // head_width
        return jnp.where(head == c * chunk_heads + of, 1.0, 0.0).astype(BF16)

    def total_decay(c):
        return ec[c, tokens - 1 : tokens, :]

    def step(s, carry):
        cf = s - SKEW * block
        cb = s - SKEW * (blocks - 1 - block)
        do_f = jnp.logical_and(cf >= 0, cf < chunks)
        do_b = jnp.logical_and(cb >= 0, cb < chunks)

        @pl.when(do_f)
        def _():
            @pl.when(has_prev)
            def _():
                forward_copy(cf).wait_recv()

            state_out[cf] = total_decay(cf) * (state_in[cf] + fresh[cf])

            @pl.when(has_next)
            def _():
                forward_copy(cf).start()

        @pl.when(do_b)
        def _():
            @pl.when(has_next)
            def _():
                backward_copy(cb).wait_recv()

            @pl.when(has_prev)
            def _():
                pull_out[cb] = total_decay(cb) * pull_in[cb] + pulled[cb]
                backward_copy(cb).start()

        @pl.when(s < chunks)
        def _():
            xs = (xs_h[s], xs_l[s])
            ys = (ys_h[s], ys_l[s])
            mt_acc[...] += dot3(xs, ys, NT)

        @pl.when(do_f)
        def _():
            entering = split(state_in[cf])
            z = joined(
                (sm[2], sm[2], sm[3], bcm[1], bcm[1]),
                (xs_h[cf], xs_l[cf], xs_h[cf], *entering),
            )
            bc_acc[1] += dot3((ys_h[cf], ys_l[cf]), entering, NT)
            v = split(ec[cf] * dyc[cf].astype(F32) * z)
            dcum_acc[...] += dot2(selector(cf), v, NT)

        @pl.when(do_b)
        def _():
            leaving = split(total_decay(cb) * pull_in[cb])
            a2 = joined(
                (sm[0], sm[0], sm[1], bcm[0], bcm[0]),
                (ys_h[cb], ys_l[cb], ys_h[cb], *leaving),
            )
            bc_acc[0] += dot3((xs_h[cb], xs_l[cb]), leaving, NT)
            x = xc[cb].astype(F32)
            growth = ed[cb]
            gx = growth * a2 + gain_row[cb, 0:1, :] * dyc[cb].astype(F32)
            gx_ref[:, pl.ds(pl.multiple_of(cb * lanes, 128), lanes)] = gx.astype(BF16)
            direct = x * a2
            pick = selector(cb)
            dir_acc[...] += dot2(pick, split(direct), NT)
            dcum_acc[...] -= dot2(pick, split(growth * direct), NT)

        return carry

    lax.fori_loop(0, chunks + SKEW * (blocks - 1), step, 0)

    inner = jnp.where(upto, mt_acc[...], 0.0)
    grad_b = bc_acc[0] + dot2l(split(inner), bcm[1])
    grad_c = bc_acc[1] + dot2l(split(inner.T), bcm[0])
    for j in range(peers):
        part[j, 0] = grad_b[j * rows : (j + 1) * rows]
        part[j, 1] = grad_c[j * rows : (j + 1) * rows]

    def sum_copy(peer, slot):
        return pltpu.make_async_remote_copy(
            src_ref=part.at[peer], dst_ref=rs.at[slot],
            send_sem=send_r.at[peer], recv_sem=recv_r.at[slot],
            device_id={"tp": peer}, device_id_type=MESH,
        )

    for d in range(1, peers):
        sum_copy(lax.rem(me + d, peers), me).start()

    edge = jnp.zeros((HEAD_PAD, 8), F32)
    for c in range(chunks):
        both = (pull_in[c] * state_out[c]).reshape(-1, 8, lanes).sum(axis=0)
        edge = edge + dot2(selector(c), split(both), NT)
    edge = jnp.sum(edge, axis=1, keepdims=True)
    after = exact(dcum_acc[...], jnp.where(row >= col, 1.0, 0.0).astype(F32)) + edge
    gstep = jnp.exp(-cums[...]) * dir_acc[...] - rates[...] * after
    gstep_ref[...] = gstep[0:head_count]

    total = part[me]
    for d in range(1, peers):
        source = lax.rem(me + d, peers)
        sum_copy(source, source).wait_recv()
        total = total + rs[source]
    gbc_ref[...] = total

    for d in range(1, peers):
        peer = lax.rem(me + d, peers)
        bc_copy(peer, me).wait_send()
        x_copy(peer, me).wait_send()
        sum_copy(peer, me).wait_send()

    def drain(c, carry):
        @pl.when(has_next)
        def _():
            forward_copy(c).wait_send()

        @pl.when(has_prev)
        def _():
            backward_copy(c).wait_send()

        return carry

    lax.fori_loop(0, chunks, drain, 0)


def shards(x_ckpt, bc_ckpt, step_sizes, decay_rate, skip_gain, grad_out):
    peers, blocks = lax.axis_size("tp"), lax.axis_size("seq")
    rows = x_ckpt.shape[0]
    head_count, tokens = step_sizes.shape
    width = grad_out.shape[1]
    state = bc_ckpt.shape[2]
    lanes = 128
    chunks = width // lanes
    head_width = width // head_count
    wide = lambda dtype, size: pltpu.VMEM((chunks, size, lanes), dtype)
    dma = lambda n: pltpu.SemaphoreType.DMA((n,))
    vmem = pl.BlockSpec(memory_space=pltpu.VMEM)
    smem = pl.BlockSpec(memory_space=pltpu.SMEM)
    heads = pltpu.VMEM((HEAD_PAD, tokens), F32)
    return pl.pallas_call(
        partial(kernel, peers, blocks, head_width),
        out_shape=(
            jax.ShapeDtypeStruct((tokens, width), BF16),
            jax.ShapeDtypeStruct((2, rows, state), F32),
            jax.ShapeDtypeStruct((head_count, tokens), F32),
        ),
        in_specs=[vmem, vmem, vmem, smem, smem, vmem],
        out_specs=(vmem, vmem, vmem),
        scratch_shapes=[
            pltpu.VMEM((peers, rows, width), BF16),
            pltpu.VMEM((peers, 2, rows, state), BF16),
            pltpu.VMEM((peers, 2, rows, state), F32),
            pltpu.VMEM((peers, 2, rows, state), F32),
            *[wide(F32, state)] * 6,
            *[wide(BF16, tokens)] * 6,
            *[wide(F32, tokens)] * 2,
            wide(F32, 8),
            heads, heads, heads, heads,
            pltpu.VMEM((tokens, tokens), F32),
            pltpu.VMEM((2, tokens, state), F32),
            heads, heads,
            pltpu.VMEM((4, tokens, tokens), BF16),
            pltpu.VMEM((2, tokens, state), BF16),
            dma(peers), dma(peers), dma(peers), dma(peers), dma(2),
            dma(chunks), dma(chunks), dma(chunks), dma(chunks),
            dma(peers), dma(peers),
        ],
        compiler_params=pltpu.CompilerParams(collective_id=0, has_side_effects=True),
    )(x_ckpt, bc_ckpt, step_sizes, decay_rate, skip_gain, grad_out)


def solution(mesh):
    return jax.shard_map(
        shards,
        mesh=mesh,
        in_specs=(
            P(("dp", "seq", "tp"), None),
            P(None, ("dp", "seq", "tp"), None),
            P("tp", ("dp", "seq")),
            P("tp"),
            P("tp"),
            P(("dp", "seq"), "tp"),
        ),
        out_specs=(
            P(("dp", "seq"), "tp"),
            P(None, ("dp", "seq", "tp"), None),
            P("tp", ("dp", "seq")),
        ),
        check_vma=False,
    )
```

```python
from functools import partial

import jax
import jax.numpy as jnp
from jax import lax
from jax.experimental import pallas as pl
from jax.experimental.pallas import tpu as pltpu
from jax.sharding import PartitionSpec as P

MESH = pl.DeviceIdType.MESH
F32 = jnp.float32
BF16 = jnp.bfloat16
HEAD_PAD = 32
SKEW = 3

NN = (((1,), (0,)), ((), ()))
NT = (((1,), (1,)), ((), ()))


def dot(a, b, dims=NN):
    return lax.dot_general(a, b, dims, preferred_element_type=F32)


def exact(a, b):
    return lax.dot_general(
        a, b, NN, precision=lax.Precision.HIGHEST, preferred_element_type=F32
    )


def split(v):
    high = v.astype(BF16)
    return high, (v - high.astype(F32)).astype(BF16)


def joined(a, b, dims=NN):
    return dot(jnp.concatenate(a, axis=1), jnp.concatenate(b, axis=dims[0][1][0]), dims)


def dot2(a, b, dims=NN):
    return joined((a, a), b, dims)


def dot2l(a, b, dims=NN):
    return joined(a, (b, b), dims)


def dot3(a, b, dims=NN):
    return joined((a[0], a[0], a[1]), (b[0], b[1], b[0]), dims)


def kernel(
    peers, blocks, head_width,
    x_ref, bc_ref, step_ref, rate_ref, gain_ref, dy_ref,
    gx_ref, gbc_ref, gstep_ref,
    xr, bcr, part, rs,
    state_in, state_out, pull_in, pull_out, fresh, pulled,
    xs_h, xs_l, ys_h, ys_l, xc, dyc, ec, ed, gain_row,
    stp, rates, gains, cums, mt_acc, bc_acc, dcum_acc, dir_acc, sm, bcm,
    send_x, recv_x, send_b, recv_b, own_sem,
    send_f, recv_f, send_g, recv_g, send_r, recv_r,
):
    me = lax.axis_index("tp")
    block = lax.axis_index("seq")
    head_count, tokens = step_ref.shape
    width = dy_ref.shape[1]
    rows = x_ref.shape[0]
    chunks, _, lanes = xc.shape
    chunk_heads = lanes // head_width

    has_prev = block > 0
    has_next = block < blocks - 1

    barrier = pltpu.get_barrier_semaphore()
    for d in range(1, peers):
        pl.semaphore_signal(
            barrier, inc=1, device_id={"tp": lax.rem(me + d, peers)}, device_id_type=MESH
        )

    @pl.when(has_prev)
    def _():
        pl.semaphore_signal(barrier, inc=1, device_id={"seq": block - 1}, device_id_type=MESH)

    @pl.when(has_next)
    def _():
        pl.semaphore_signal(barrier, inc=1, device_id={"seq": block + 1}, device_id_type=MESH)

    neighbours = jnp.where(has_prev, 1, 0) + jnp.where(has_next, 1, 0)
    pl.semaphore_wait(barrier, peers - 1 + neighbours)

    def bc_copy(peer, slot):
        return pltpu.make_async_remote_copy(
            src_ref=bc_ref, dst_ref=bcr.at[slot],
            send_sem=send_b.at[peer], recv_sem=recv_b.at[slot],
            device_id={"tp": peer}, device_id_type=MESH,
        )

    def x_copy(peer, slot):
        return pltpu.make_async_remote_copy(
            src_ref=x_ref.at[:, pl.ds(pl.multiple_of(peer * width, 128), width)],
            dst_ref=xr.at[slot],
            send_sem=send_x.at[peer], recv_sem=recv_x.at[slot],
            device_id={"tp": peer}, device_id_type=MESH,
        )

    for d in range(1, peers):
        bc_copy(lax.rem(me + d, peers), me).start()
    for d in range(1, peers):
        x_copy(lax.rem(me + d, peers), me).start()
    own_x = pltpu.make_async_copy(
        x_ref.at[:, pl.ds(pl.multiple_of(me * width, 128), width)], xr.at[me], own_sem.at[0]
    )
    own_bc = pltpu.make_async_copy(bc_ref, bcr.at[me], own_sem.at[1])
    own_x.start()
    own_bc.start()

    stp[...] = jnp.zeros_like(stp)
    stp[0:head_count] = step_ref[...]
    rates[...] = jnp.zeros_like(rates)
    gains[...] = jnp.zeros_like(gains)
    for h in range(head_count):
        rates[h : h + 1] = jnp.full((1, tokens), rate_ref[h], F32)
        gains[h : h + 1] = jnp.full((1, tokens), gain_ref[h], F32)
    row = lax.broadcasted_iota(jnp.int32, (tokens, tokens), 0)
    col = lax.broadcasted_iota(jnp.int32, (tokens, tokens), 1)
    upto = row <= col
    cum = exact(-rates[...] * stp[...], jnp.where(upto, 1.0, 0.0).astype(F32))
    cums[...] = cum
    stacked = jnp.concatenate(
        [jnp.exp(cum), jnp.exp(-cum) * stp[...], gains[...], jnp.zeros_like(cum)], axis=0
    )
    table = split(stacked.T)
    pick_row = lax.broadcasted_iota(jnp.int32, (4 * HEAD_PAD, lanes), 0)
    pick_head = lax.broadcasted_iota(jnp.int32, (4 * HEAD_PAD, lanes), 1) // head_width
    for c in range(chunks):
        def spread(q):
            hit = pick_row == (q * HEAD_PAD + c * chunk_heads) + pick_head
            return jnp.where(hit, 1.0, 0.0).astype(BF16)

        grown = dot2l(table, spread(0))
        ec[c] = grown
        ed[c] = dot2l(table, spread(1))
        gain_row[c] = dot2l((table[0][0:16], table[1][0:16]), spread(2))[0:8]
        dy = dy_ref[:, c * lanes : (c + 1) * lanes]
        dyc[c] = dy
        high, low = split(grown * dy.astype(F32))
        ys_h[c] = high
        ys_l[c] = low

    own_bc.wait()
    for d in range(1, peers):
        source = lax.rem(me + d, peers)
        bc_copy(source, source).wait_recv()
    proj_b = bcr[:, 0].reshape(tokens, -1)
    proj_c = bcr[:, 1].reshape(tokens, -1)
    bcm[0] = proj_b
    bcm[1] = proj_c
    b_t = proj_b.astype(F32).T.astype(BF16)
    c_t = proj_c.astype(F32).T.astype(BF16)
    scores_t = jnp.where(upto, dot(proj_b, proj_c, NT), 0.0)
    sm[0], sm[1] = split(scores_t)
    sm[2], sm[3] = split(scores_t.T)
    for c in range(chunks):
        pulled[c] = dot2(c_t, (ys_h[c], ys_l[c]))

    @pl.when(jnp.logical_not(has_prev))
    def _():
        state_in[...] = jnp.zeros_like(state_in)

    @pl.when(jnp.logical_not(has_next))
    def _():
        pull_in[...] = jnp.zeros_like(pull_in)

    mt_acc[...] = jnp.zeros_like(mt_acc)
    bc_acc[...] = jnp.zeros_like(bc_acc)
    dcum_acc[...] = jnp.zeros_like(dcum_acc)
    dir_acc[...] = jnp.zeros_like(dir_acc)

    own_x.wait()
    for d in range(1, peers):
        source = lax.rem(me + d, peers)
        x_copy(source, source).wait_recv()
    for c in range(chunks):
        x = xr[:, :, c * lanes : (c + 1) * lanes].reshape(tokens, lanes)
        xc[c] = x
        pair = split(ed[c] * x.astype(F32))
        xs_h[c] = pair[0]
        xs_l[c] = pair[1]
        fresh[c] = dot2(b_t, pair)

    def forward_copy(c):
        return pltpu.make_async_remote_copy(
            src_ref=state_out.at[c], dst_ref=state_in.at[c],
            send_sem=send_f.at[c], recv_sem=recv_f.at[c],
            device_id={"seq": block + 1}, device_id_type=MESH,
        )

    def backward_copy(c):
        return pltpu.make_async_remote_copy(
            src_ref=pull_out.at[c], dst_ref=pull_in.at[c],
            send_sem=send_g.at[c], recv_sem=recv_g.at[c],
            device_id={"seq": block - 1}, device_id_type=MESH,
        )

    def selector(c):
        head = lax.broadcasted_iota(jnp.int32, (HEAD_PAD, lanes), 0)
        of = lax.broadcasted_iota(jnp.int32, (HEAD_PAD, lanes), 1) // head_width
        return jnp.where(head == c * chunk_heads + of, 1.0, 0.0).astype(BF16)

    def total_decay(c):
        return ec[c, tokens - 1 : tokens, :]

    def step(s, carry):
        cf = s - SKEW * block
        cb = s - SKEW * (blocks - 1 - block)
        do_f = jnp.logical_and(cf >= 0, cf < chunks)
        do_b = jnp.logical_and(cb >= 0, cb < chunks)

        @pl.when(do_f)
        def _():
            @pl.when(has_prev)
            def _():
                forward_copy(cf).wait_recv()

            state_out[cf] = total_decay(cf) * (state_in[cf] + fresh[cf])

            @pl.when(has_next)
            def _():
                forward_copy(cf).start()

        @pl.when(do_b)
        def _():
            @pl.when(has_next)
            def _():
                backward_copy(cb).wait_recv()

            @pl.when(has_prev)
            def _():
                pull_out[cb] = total_decay(cb) * pull_in[cb] + pulled[cb]
                backward_copy(cb).start()

        @pl.when(s < chunks)
        def _():
            xs = (xs_h[s], xs_l[s])
            ys = (ys_h[s], ys_l[s])
            mt_acc[...] += dot3(xs, ys, NT)

        @pl.when(do_f)
        def _():
            entering = split(state_in[cf])
            z = joined(
                (sm[2], sm[2], sm[3], bcm[1], bcm[1]),
                (xs_h[cf], xs_l[cf], xs_h[cf], *entering),
            )
            bc_acc[1] += dot3((ys_h[cf], ys_l[cf]), entering, NT)
            v = split(ec[cf] * dyc[cf].astype(F32) * z)
            dcum_acc[...] += dot2(selector(cf), v, NT)

        @pl.when(do_b)
        def _():
            leaving = split(total_decay(cb) * pull_in[cb])
            a2 = joined(
                (sm[0], sm[0], sm[1], bcm[0], bcm[0]),
                (ys_h[cb], ys_l[cb], ys_h[cb], *leaving),
            )
            bc_acc[0] += dot3((xs_h[cb], xs_l[cb]), leaving, NT)
            x = xc[cb].astype(F32)
            growth = ed[cb]
            gx = growth * a2 + gain_row[cb, 0:1, :] * dyc[cb].astype(F32)
            gx_ref[:, pl.ds(pl.multiple_of(cb * lanes, 128), lanes)] = gx.astype(BF16)
            direct = x * a2
            pick = selector(cb)
            dir_acc[...] += dot2(pick, split(direct), NT)
            dcum_acc[...] -= dot2(pick, split(growth * direct), NT)

        return carry

    lax.fori_loop(0, chunks + SKEW * (blocks - 1), step, 0)

    inner = jnp.where(upto, mt_acc[...], 0.0)
    grad_b = bc_acc[0] + dot2l(split(inner), bcm[1])
    grad_c = bc_acc[1] + dot2l(split(inner.T), bcm[0])
    for j in range(peers):
        part[j, 0] = grad_b[j * rows : (j + 1) * rows]
        part[j, 1] = grad_c[j * rows : (j + 1) * rows]

    def sum_copy(peer, slot):
        return pltpu.make_async_remote_copy(
            src_ref=part.at[peer], dst_ref=rs.at[slot],
            send_sem=send_r.at[peer], recv_sem=recv_r.at[slot],
            device_id={"tp": peer}, device_id_type=MESH,
        )

    for d in range(1, peers):
        sum_copy(lax.rem(me + d, peers), me).start()

    edge = jnp.zeros((HEAD_PAD, 8), F32)
    for c in range(chunks):
        both = (pull_in[c] * state_out[c]).reshape(-1, 8, lanes).sum(axis=0)
        edge = edge + dot2(selector(c), split(both), NT)
    edge = jnp.sum(edge, axis=1, keepdims=True)
    after = exact(dcum_acc[...], jnp.where(row >= col, 1.0, 0.0).astype(F32)) + edge
    gstep = jnp.exp(-cums[...]) * dir_acc[...] - rates[...] * after
    gstep_ref[...] = gstep[0:head_count]

    total = part[me]
    for d in range(1, peers):
        source = lax.rem(me + d, peers)
        sum_copy(source, source).wait_recv()
        total = total + rs[source]
    gbc_ref[...] = total

    for d in range(1, peers):
        peer = lax.rem(me + d, peers)
        bc_copy(peer, me).wait_send()
        x_copy(peer, me).wait_send()
        sum_copy(peer, me).wait_send()

    def drain(c, carry):
        @pl.when(has_next)
        def _():
            forward_copy(c).wait_send()

        @pl.when(has_prev)
        def _():
            backward_copy(c).wait_send()

        return carry

    lax.fori_loop(0, chunks, drain, 0)


def shards(x_ckpt, bc_ckpt, step_sizes, decay_rate, skip_gain, grad_out):
    peers, blocks = lax.axis_size("tp"), lax.axis_size("seq")
    rows = x_ckpt.shape[0]
    head_count, tokens = step_sizes.shape
    width = grad_out.shape[1]
    state = bc_ckpt.shape[2]
    lanes = 128
    chunks = width // lanes
    head_width = width // head_count
    wide = lambda dtype, size: pltpu.VMEM((chunks, size, lanes), dtype)
    dma = lambda n: pltpu.SemaphoreType.DMA((n,))
    vmem = pl.BlockSpec(memory_space=pltpu.VMEM)
    smem = pl.BlockSpec(memory_space=pltpu.SMEM)
    heads = pltpu.VMEM((HEAD_PAD, tokens), F32)
    return pl.pallas_call(
        partial(kernel, peers, blocks, head_width),
        out_shape=(
            jax.ShapeDtypeStruct((tokens, width), BF16),
            jax.ShapeDtypeStruct((2, rows, state), F32),
            jax.ShapeDtypeStruct((head_count, tokens), F32),
        ),
        in_specs=[vmem, vmem, vmem, smem, smem, vmem],
        out_specs=(vmem, vmem, vmem),
        scratch_shapes=[
            pltpu.VMEM((peers, rows, width), BF16),
            pltpu.VMEM((peers, 2, rows, state), BF16),
            pltpu.VMEM((peers, 2, rows, state), F32),
            pltpu.VMEM((peers, 2, rows, state), F32),
            *[wide(F32, state)] * 6,
            *[wide(BF16, tokens)] * 6,
            *[wide(F32, tokens)] * 2,
            wide(F32, 8),
            heads, heads, heads, heads,
            pltpu.VMEM((tokens, tokens), F32),
            pltpu.VMEM((2, tokens, state), F32),
            heads, heads,
            pltpu.VMEM((4, tokens, tokens), BF16),
            pltpu.VMEM((2, tokens, state), BF16),
            dma(peers), dma(peers), dma(peers), dma(peers), dma(2),
            dma(chunks), dma(chunks), dma(chunks), dma(chunks),
            dma(peers), dma(peers),
        ],
        compiler_params=pltpu.CompilerParams(collective_id=0, has_side_effects=True),
    )(x_ckpt, bc_ckpt, step_sizes, decay_rate, skip_gain, grad_out)


def solution(mesh):
    return jax.shard_map(
        shards,
        mesh=mesh,
        in_specs=(
            P(("dp", "seq", "tp"), None),
            P(None, ("dp", "seq", "tp"), None),
            P("tp", ("dp", "seq")),
            P("tp"),
            P("tp"),
            P(("dp", "seq"), "tp"),
        ),
        out_specs=(
            P(("dp", "seq"), "tp"),
            P(None, ("dp", "seq", "tp"), None),
            P("tp", ("dp", "seq")),
        ),
        check_vma=False,
    )
```
